32 devices in a mesh: group: 2 (over y), expert: 4 (over z), tensor: 2 (over x), sub: 2 (over core).
Axes of the slice: x: 2, y: 2, z: 4, core: 2. Of those that a mesh axis runs over, the one named last changes fastest.
Arguments:
- tokens: bfloat16 [64, 7168], P(('group', 'expert', 'sub')), parts along dimension 0, may hold values from -6 to 6
- expert_ids: int32 [64, 2], P(('group', 'expert', 'sub')), parts along dimension 0, may hold values from 0 to 1, all different within a row; in each aligned block of 4 rows (0 to 3, 4 to 7, ...) at most 4 rows name the same one
- gate_codes: int32 [64, 2], P(('group', 'expert', 'sub')), parts along dimension 0, may hold values from 1 to 63
- w_gate: bfloat16 [4, 1024, 7168], P('expert', ('tensor', 'sub')), may hold values from -0.0625 to 0.0625
- w_up: bfloat16 [4, 1024, 7168], P('expert', ('tensor', 'sub')), may hold values from -0.0625 to 0.0625
- w_down: bfloat16 [4, 1024, 7168], P('expert', ('tensor', 'sub')), may hold values from -0.125 to 0.125
Outputs:
- mixed: bfloat16 [64, 7168], P(('group', 'expert', 'sub'), 'tensor'), parts along dimension 0
The draws below stay inside these ranges and needn't reach their ends.
There are 2 independent parts, one for each index of `group`. The reference program is written for one: setup_inputs(seed, part) draws one part's arguments, and reference() takes and returns one part's arrays. A program takes and returns all parts, laid end to end along the dimension named above; an argument that names none is the same for every part. Nothing has to cross between parts.
Inputs may be any that keep to these rules, and one draw needn't show every extreme that they name: `expert_ids`: the 2 numbers of a row differ; within the rows of one device (aligned blocks of 4 rows) no expert is named by more than 4 rows, a bound that some block reaches.
All inputs are finite; a program needn't handle non-finite values.
Results may differ from the reference program's by a relative error of at most 0.008.
Values may be sent and summed in bfloat16 or wider, within the bound.
A program may use at most 64 MiB of HBM per device.

```python
import math
import jax
import jax.numpy as jnp
import numpy as np
from jax import lax

D = 7168
FF = 2048
TOK_DEV = 4
EXPERTS = 2
HALVES = 4
TOP = 2
CAP = 4
RUN = 256
TOKENS = 32


def set_ends(drawn, rng, smallest, high):
    spot = [jax.random.randint(jax.random.fold_in(rng, axis), (), 0, length) for axis, length in enumerate(drawn.shape)]
    widest = drawn.shape.index(max(drawn.shape))
    next_to = spot[:widest] + [(spot[widest] + 1) % drawn.shape[widest]] + spot[widest + 1:]
    return drawn.at[tuple(spot)].set(smallest).at[tuple(next_to)].set(high)


def block_scale(key, extent, cuts, low, top_value):
    def one(position, parts):
        steps = jax.random.uniform(jax.random.fold_in(jax.random.fold_in(key, 6), position), (parts,), jnp.float32, low / len(cuts), top_value / len(cuts))
        return jnp.repeat(jnp.exp(steps), extent[position] // parts).reshape((-1,) + (1,) * (len(extent) - position - 1))

    factor_of = one(*cuts[0])
    for cut in cuts[1:]:
        factor_of = factor_of * one(*cut)
    return factor_of


def deal_out(key, own, number, rows, count, top, bound, lean):
    ranking = jax.random.permutation(key, count)
    heavy_load, usual = load_shares(count, rows * top, bound, lean, True), load_shares(count, rows * top, bound, lean, False)
    places = jnp.arange(count)

    def named(tallies, turn):
        used = int((tallies > 0).sum())
        fixed = max(1, used // 4)
        moved = fixed + (places - fixed + turn * (used - fixed)) % max(1, count - fixed)
        return jnp.zeros((count,), jnp.int32).at[ranking[jnp.where(places < fixed, places, moved)]].set(jnp.asarray(tallies, jnp.int32))

    tallies = jnp.where(number % 4 == 0, named(heavy_load, number // 4), named(usual, number - number // 4 - 1))
    mixed = jax.random.permutation(jax.random.fold_in(own, 3), count)
    giver, receiver = mixed[0:count // 2 * 2:2], mixed[1:count // 2 * 2:2]
    slack = jnp.minimum(tallies[giver] - 1, bound - tallies[receiver]) // 2
    slack = jnp.where((giver == ranking[0]) | (receiver == ranking[0]) | (tallies[receiver] == 0), 0, jnp.maximum(slack, 0))
    moved = jax.random.randint(jax.random.fold_in(own, 4), (count // 2,), 0, 1 << 20) % (slack + 1)
    tallies = tallies.at[giver].add(-moved).at[receiver].add(moved)
    items = jnp.searchsorted(jnp.cumsum(tallies), jnp.arange(rows * top), side="right").astype(jnp.int32)
    table = items.reshape(top, rows).T
    table = table[jax.random.permutation(jax.random.fold_in(own, 1), rows)]
    turn = jax.random.randint(jax.random.fold_in(own, 2), (rows, 1), 0, top)
    return jnp.take_along_axis(table, (jnp.arange(top)[None, :] + turn) % top, axis=1)


def load_shares(count, total, bound, skew, full):
    loads = [(1 << 20) // math.isqrt(rank ** skew) + 1 for rank in range(1, count + 1)]
    largest = bound if full else min(bound, max(-(-total // count), total * loads[0] // sum(loads)))
    least = 1 if total - largest >= count - 1 else 0
    counts, spare = [largest] + [least] * (count - 1), total - largest - least * (count - 1)
    while spare > 0:
        candidates = [i for i in range(1, count) if counts[i] < largest] or [i for i in range(1, count) if counts[i] < bound]
        pool, left = sum([loads[i] for i in candidates]), spare
        for i in candidates:
            more = min(bound - counts[i], max(1, left * loads[i] // pool), spare)
            counts[i] = counts[i] + more
            spare = spare - more
    return np.array(counts)


def normal_values(own_key, dims, deviation, most, pieces=(), held_as=jnp.bfloat16):
    gain = block_scale(own_key, dims, pieces, -0.22, 0.18) if pieces else 1.0
    drawn = jax.random.normal(own_key, dims, jnp.float32) * deviation * gain
    return jnp.minimum(jnp.maximum(drawn, -most), most).astype(held_as)


def setup_inputs(seed: int = 0, part: int = 0) -> dict:
    arg_keys = jax.random.split(jax.random.key(seed), 7)
    part_keys = jax.random.split(jax.random.fold_in(arg_keys[6], part), 7)
    tokens = normal_values(part_keys[0], (TOKENS, D), 1.0, 6.0, ((0, 8),))
    expert_ids_keys = jax.random.split(jax.random.fold_in(part_keys[1], 1), TOKENS // TOK_DEV)
    expert_ids_turns = jax.random.permutation(jax.random.fold_in(part_keys[1], 3), TOKENS // TOK_DEV)
    expert_ids = jax.vmap(lambda own, number: deal_out(jax.random.fold_in(part_keys[1], 2), own, number, TOK_DEV, EXPERTS, TOP, CAP, 1))(expert_ids_keys, expert_ids_turns).reshape((TOKENS, TOP))
    gate_codes = set_ends(jax.random.randint(part_keys[2], (TOKENS, TOP), 1, 64), jax.random.fold_in(part_keys[2], 1), 1, 63).astype(jnp.int32)
    w_gate = normal_values(arg_keys[3], (HALVES, FF // 2, D), D ** -0.5, 0.0625, ((0, 4), (1, 4)))
    w_up = normal_values(arg_keys[4], (HALVES, FF // 2, D), D ** -0.5, 0.0625, ((0, 4), (1, 4)))
    w_down = normal_values(arg_keys[5], (HALVES, FF // 2, D), FF ** -0.5, 0.125, ((0, 4), (1, 4)))
    return dict(tokens=tokens, expert_ids=expert_ids, gate_codes=gate_codes, w_gate=w_gate, w_up=w_up, w_down=w_down)


def reference(tokens, expert_ids, gate_codes, w_gate, w_up, w_down):
    weight = gate_codes.astype(jnp.float32) / 64.0
    token_count = tokens.shape[0]
    run_count = FF // RUN
    contract = (((1,), (1,)), ((), ()))

    def one_expert(total_out, expert):
        gate_full = jnp.concatenate([w_gate[2 * expert], w_gate[2 * expert + 1]], axis=0)
        up_full = jnp.concatenate([w_up[2 * expert], w_up[2 * expert + 1]], axis=0)
        down_full = jnp.concatenate([w_down[2 * expert], w_down[2 * expert + 1]], axis=0)
        gate_act = lax.dot_general(tokens, gate_full, contract, preferred_element_type=jnp.float32)
        up_act = lax.dot_general(tokens, up_full, contract, preferred_element_type=jnp.float32)
        hidden = (jax.nn.silu(gate_act) * up_act).astype(jnp.bfloat16)
        hid_runs = hidden.reshape(token_count, run_count, RUN).transpose(1, 0, 2)
        down_runs = down_full.reshape(run_count, RUN, D)

        def add_run(running, run_pair):
            hid_run, down_run = run_pair
            piece = jnp.dot(hid_run, down_run, preferred_element_type=jnp.float32).astype(jnp.bfloat16)
            piece = lax.optimization_barrier(piece)
            return running + piece.astype(jnp.float32), None

        summed, _ = lax.scan(add_run, jnp.zeros((token_count, D), jnp.float32), (hid_runs, down_runs))
        share_of = jnp.sum(jnp.where(expert_ids == expert, weight, jnp.float32(0.0)), axis=1)
        return total_out + share_of[:, None] * summed, None

    total_out, _ = lax.scan(one_expert, jnp.zeros((token_count, D), jnp.float32), jnp.arange(EXPERTS, dtype=jnp.int32))
    return total_out.astype(jnp.bfloat16)
```

```python
import functools

import jax
import jax.numpy as jnp
from jax import lax
from jax.experimental import pallas as pl
from jax.experimental.pallas import tpu as pltpu
from jax.sharding import PartitionSpec as P

MESH = pl.DeviceIdType.MESH


def split_count(width, most):
    parts = most
    while width % (parts * 128):
        parts -= 1
    return parts


def layer(
    E, X, K, C,
    tok_hbm, ids_hbm, codes_hbm, wg_hbm, wu_hbm, wd_hbm,
    out_ref,
    gat, xs, ids_v, codes_v, wg, wu, wd,
    keep, d_out, d_in, b_out, b_in, c_out, c_in,
    small_sem, wg_sem, wu_sem, wd_sem,
    z_send, z_recv, f_send, f_recv, d_send, d_recv, b_send, b_recv, c_send, c_recv,
):
    T, D = tok_hbm.shape
    half = E * T
    kw = D // K
    block = D // X
    cw = block // C
    e = lax.axis_index("expert")
    x = lax.axis_index("tensor")
    s = lax.axis_index("sub")
    partner = {"sub": 1 - s}

    tok_copy = pltpu.make_async_copy(tok_hbm, gat.at[0, e], small_sem.at[0])
    tok_copy.start()
    ids_copy = pltpu.make_async_copy(ids_hbm, ids_v, small_sem.at[1])
    codes_copy = pltpu.make_async_copy(codes_hbm, codes_v, small_sem.at[2])
    ids_copy.start()
    codes_copy.start()

    barrier = pltpu.get_barrier_semaphore()
    for d in range(1, E):
        pl.semaphore_signal(barrier, inc=1, device_id={"expert": (e + d) % E}, device_id_type=MESH)
    for d in range(1, X):
        pl.semaphore_signal(barrier, inc=1, device_id={"tensor": (x + d) % X}, device_id_type=MESH)
    pl.semaphore_signal(barrier, inc=1, device_id=partner, device_id_type=MESH)

    g_copies, u_copies, w_copies = [], [], {}
    for k in range(K):
        cols = pl.ds(k * kw, kw)
        g_copies.append(pltpu.make_async_copy(wg_hbm.at[0, :, cols], wg.at[k], wg_sem.at[k]))
        u_copies.append(pltpu.make_async_copy(wu_hbm.at[0, :, cols], wu.at[k], wu_sem.at[k]))
        g_copies[k].start()
        u_copies[k].start()
    order = [(i, c) for i in list(range(1, X)) + [0] for c in range(C)]
    for i, c in order:
        first = pl.multiple_of(((x + i) % X) * block + c * cw, 128)
        w_copies[i, c] = pltpu.make_async_copy(
            wd_hbm.at[0, :, pl.ds(first, cw)], wd.at[i, c], wd_sem.at[i, c]
        )
        w_copies[i, c].start()

    tok_copy.wait()
    pl.semaphore_wait(barrier, E - 1 + X - 1 + 1)

    def z_copy(d, k, slot):
        piece = gat.at[0, slot, :, pl.ds(k * kw, kw)]
        return pltpu.make_async_remote_copy(
            src_ref=piece, dst_ref=piece, send_sem=z_send.at[d, k], recv_sem=z_recv.at[d, k],
            device_id={"expert": (e + d) % E}, device_id_type=MESH,
        )

    def f_copy(d, k):
        slot = (e + E - d) % E
        cols = pl.ds(k * kw, kw)
        return pltpu.make_async_remote_copy(
            src_ref=gat.at[0, slot, :, cols], dst_ref=gat.at[1, slot, :, cols],
            send_sem=f_send.at[d, k], recv_sem=f_recv.at[d, k],
            device_id=partner, device_id_type=MESH,
        )

    sent = []
    for k in range(K):
        for d in range(1, E):
            copy = z_copy(d, k, e)
            copy.start()
            sent.append(copy)
        copy = f_copy(0, k)
        copy.start()
        sent.append(copy)

    def forward(k):
        for d in range(1, E):
            z_copy(d, k, (e + E - d) % E).wait_recv()
            copy = f_copy(d, k)
            copy.start()
            sent.append(copy)

    contract = (((1,), (1,)), ((), ()))
    gate_act = up_act = None
    forward(0)
    for k in range(K):
        if k + 1 < K:
            forward(k + 1)
        for d in range(E):
            f_copy(d, k).wait_recv()
        for r in range(2):
            for j in range(E):
                xs[pl.ds((r * E + j) * T, T), pl.ds(k * kw, kw)] = gat[r, j, :, pl.ds(k * kw, kw)]
        rows = xs[:, pl.ds(k * kw, kw)]
        g_copies[k].wait()
        gate_part = lax.dot_general(rows, wg[k], contract, preferred_element_type=jnp.float32)
        u_copies[k].wait()
        up_part = lax.dot_general(rows, wu[k], contract, preferred_element_type=jnp.float32)
        gate_act = gate_part if k == 0 else gate_act + gate_part
        up_act = up_part if k == 0 else up_act + up_part
    hidden = (gate_act / (1.0 + jnp.exp(-gate_act)) * up_act).astype(jnp.bfloat16)

    def d_copy(i, c):
        return pltpu.make_async_remote_copy(
            src_ref=d_out.at[i, c], dst_ref=d_in.at[i, c],
            send_sem=d_send.at[i, c], recv_sem=d_recv.at[i, c],
            device_id=partner, device_id_type=MESH,
        )

    def b_copy(i, c):
        return pltpu.make_async_remote_copy(
            src_ref=b_out.at[i, c], dst_ref=b_in.at[i, c],
            send_sem=b_send.at[i, c], recv_sem=b_recv.at[i, c],
            device_id={"tensor": (x + i) % X}, device_id_type=MESH,
        )

    def c_copy(d, c):
        return pltpu.make_async_remote_copy(
            src_ref=c_out.at[(e + d) % E, c], dst_ref=c_in.at[d, c],
            send_sem=c_send.at[d, c], recv_sem=c_recv.at[d, c],
            device_id={"expert": (e + d) % E}, device_id_type=MESH,
        )

    def down(i, c):
        w_copies[i, c].wait()
        piece = jnp.dot(hidden, wd[i, c], preferred_element_type=jnp.float32)
        d_out[i, c] = piece[half:].astype(jnp.bfloat16)
        copy = d_copy(i, c)
        copy.start()
        sent.append(copy)
        keep[i, c] = piece[:half]

    def over_tensor(i, c):
        d_copy(i, c).wait_recv()
        both = keep[i, c] + d_in[i, c].astype(jnp.float32)
        if i:
            b_out[i, c] = both.astype(jnp.bfloat16)
            copy = b_copy(i, c)
            copy.start()
            sent.append(copy)
        else:
            for d in range(1, X):
                b_copy(d, c).wait_recv()
                both = both + b_in[d, c].astype(jnp.float32)
            both = both.astype(jnp.bfloat16)
            for j in range(E):
                c_out[j, c] = both[j * T:(j + 1) * T]
            for d in range(1, E):
                copy = c_copy(d, c)
                copy.start()
                sent.append(copy)

    down(*order[0])
    for n in range(1, len(order)):
        down(*order[n])
        over_tensor(*order[n - 1])
    over_tensor(*order[-1])

    ids_copy.wait()
    codes_copy.wait()
    weight = codes_v[...].astype(jnp.float32) / 64.0
    shares = []
    for d in range(E):
        expert = ((e + E - d) % E) // 2
        shares.append(jnp.sum(jnp.where(ids_v[...] == expert, weight, 0.0), axis=1, keepdims=True))
    for c in range(C):
        total = shares[0] * c_out[e, c].astype(jnp.float32)
        for d in range(1, E):
            c_copy(d, c).wait_recv()
            total = total + shares[d] * c_in[d, c].astype(jnp.float32)
        out_ref[:, pl.ds(c * cw, cw)] = total.astype(jnp.bfloat16)
    for copy in sent:
        copy.wait_send()


def shards(tokens, expert_ids, gate_codes, w_gate, w_up, w_down):
    T, D = tokens.shape
    E = lax.axis_size("expert")
    X = lax.axis_size("tensor")
    F = w_gate.shape[1]
    K = split_count(D, 4)
    block = D // X
    C = split_count(block, 2)
    kw, cw = D // K, block // C
    half = E * T
    bf16, f32 = jnp.bfloat16, jnp.float32
    dma = pltpu.SemaphoreType.DMA
    hbm = pl.BlockSpec(memory_space=pl.ANY)
    return pl.pallas_call(
        functools.partial(layer, E, X, K, C),
        out_shape=jax.ShapeDtypeStruct((T, block), bf16),
        in_specs=[hbm] * 6,
        out_specs=pl.BlockSpec(memory_space=pltpu.VMEM),
        scratch_shapes=[
            pltpu.VMEM((2, E, T, D), bf16),
            pltpu.VMEM((2 * half, D), bf16),
            pltpu.VMEM(expert_ids.shape, jnp.int32),
            pltpu.VMEM(gate_codes.shape, jnp.int32),
            pltpu.VMEM((K, F, kw), bf16),
            pltpu.VMEM((K, F, kw), bf16),
            pltpu.VMEM((X, C, F, cw), bf16),
            pltpu.VMEM((X, C, half, cw), f32),
            pltpu.VMEM((X, C, half, cw), bf16),
            pltpu.VMEM((X, C, half, cw), bf16),
            pltpu.VMEM((X, C, half, cw), bf16),
            pltpu.VMEM((X, C, half, cw), bf16),
            pltpu.VMEM((E, C, T, cw), bf16),
            pltpu.VMEM((E, C, T, cw), bf16),
            dma((3,)), dma((K,)), dma((K,)), dma((X, C)),
            dma((E, K)), dma((E, K)), dma((E, K)), dma((E, K)),
            dma((X, C)), dma((X, C)), dma((X, C)), dma((X, C)),
            dma((E, C)), dma((E, C)),
        ],
        compiler_params=pltpu.CompilerParams(
            collective_id=0, has_side_effects=True, vmem_limit_bytes=56 * 1024 * 1024
        ),
    )(tokens, expert_ids, gate_codes, w_gate, w_up, w_down)


def solution(mesh):
    return jax.shard_map(
        shards,
        mesh=mesh,
        in_specs=(
            P(("group", "expert", "sub"), None),
            P(("group", "expert", "sub"), None),
            P(("group", "expert", "sub"), None),
            P("expert", ("tensor", "sub"), None),
            P("expert", ("tensor", "sub"), None),
            P("expert", ("tensor", "sub"), None),
        ),
        out_specs=P(("group", "expert", "sub"), "tensor"),
        check_vma=False,
    )
```

```python
import functools

import jax
import jax.numpy as jnp
from jax import lax
from jax.experimental import pallas as pl
from jax.experimental.pallas import tpu as pltpu
from jax.sharding import PartitionSpec as P

MESH = pl.DeviceIdType.MESH


def split_count(width, most):
    parts = most
    while width % (parts * 128):
        parts -= 1
    return parts


def layer(
    E, X, K, C,
    tok_hbm, ids_hbm, codes_hbm, wg_hbm, wu_hbm, wd_hbm,
    out_ref,
    gat, xs, ids_v, codes_v, wg, wu, wd,
    keep, d_out, d_in, b_out, b_in, c_out, c_in,
    small_sem, wg_sem, wu_sem, wd_sem,
    z_send, z_recv, f_send, f_recv, d_send, d_recv, b_send, b_recv, c_send, c_recv,
):
    T, D = tok_hbm.shape
    half = E * T
    kw = D // K
    block = D // X
    cw = block // C
    e = lax.axis_index("expert")
    x = lax.axis_index("tensor")
    s = lax.axis_index("sub")
    partner = {"sub": 1 - s}

    tok_copy = pltpu.make_async_copy(tok_hbm, gat.at[0, e], small_sem.at[0])
    tok_copy.start()
    ids_copy = pltpu.make_async_copy(ids_hbm, ids_v, small_sem.at[1])
    codes_copy = pltpu.make_async_copy(codes_hbm, codes_v, small_sem.at[2])
    ids_copy.start()
    codes_copy.start()

    barrier = pltpu.get_barrier_semaphore()
    for d in range(1, E):
        pl.semaphore_signal(barrier, inc=1, device_id={"expert": (e + d) % E}, device_id_type=MESH)
    for d in range(1, X):
        pl.semaphore_signal(barrier, inc=1, device_id={"tensor": (x + d) % X}, device_id_type=MESH)
    pl.semaphore_signal(barrier, inc=1, device_id=partner, device_id_type=MESH)

    g_copies, u_copies, w_copies = [], [], {}
    for k in range(K):
        cols = pl.ds(k * kw, kw)
        g_copies.append(pltpu.make_async_copy(wg_hbm.at[0, :, cols], wg.at[k], wg_sem.at[k]))
        u_copies.append(pltpu.make_async_copy(wu_hbm.at[0, :, cols], wu.at[k], wu_sem.at[k]))
        g_copies[k].start()
        u_copies[k].start()
    order = [(i, c) for i in list(range(1, X)) + [0] for c in range(C)]
    for i, c in order:
        first = pl.multiple_of(((x + i) % X) * block + c * cw, 128)
        w_copies[i, c] = pltpu.make_async_copy(
            wd_hbm.at[0, :, pl.ds(first, cw)], wd.at[i, c], wd_sem.at[i, c]
        )
        w_copies[i, c].start()

    tok_copy.wait()
    pl.semaphore_wait(barrier, E - 1 + X - 1 + 1)

    def z_copy(d, k, slot):
        piece = gat.at[0, slot, :, pl.ds(k * kw, kw)]
        return pltpu.make_async_remote_copy(
            src_ref=piece, dst_ref=piece, send_sem=z_send.at[d, k], recv_sem=z_recv.at[d, k],
            device_id={"expert": (e + d) % E}, device_id_type=MESH,
        )

    def f_copy(d, k):
        slot = (e + E - d) % E
        cols = pl.ds(k * kw, kw)
        return pltpu.make_async_remote_copy(
            src_ref=gat.at[0, slot, :, cols], dst_ref=gat.at[1, slot, :, cols],
            send_sem=f_send.at[d, k], recv_sem=f_recv.at[d, k],
            device_id=partner, device_id_type=MESH,
        )

    sent = []
    for k in range(K):
        for d in range(1, E):
            copy = z_copy(d, k, e)
            copy.start()
            sent.append(copy)
        copy = f_copy(0, k)
        copy.start()
        sent.append(copy)

    def forward(k):
        for d in range(1, E):
            z_copy(d, k, (e + E - d) % E).wait_recv()
            copy = f_copy(d, k)
            copy.start()
            sent.append(copy)

    contract = (((1,), (1,)), ((), ()))
    gate_act = up_act = None
    forward(0)
    for k in range(K):
        if k + 1 < K:
            forward(k + 1)
        for d in range(E):
            f_copy(d, k).wait_recv()
        for r in range(2):
            for j in range(E):
                xs[pl.ds((r * E + j) * T, T), pl.ds(k * kw, kw)] = gat[r, j, :, pl.ds(k * kw, kw)]
        rows = xs[:, pl.ds(k * kw, kw)]
        g_copies[k].wait()
        gate_part = lax.dot_general(rows, wg[k], contract, preferred_element_type=jnp.float32)
        u_copies[k].wait()
        up_part = lax.dot_general(rows, wu[k], contract, preferred_element_type=jnp.float32)
        gate_act = gate_part if k == 0 else gate_act + gate_part
        up_act = up_part if k == 0 else up_act + up_part
    hidden = (gate_act / (1.0 + jnp.exp(-gate_act)) * up_act).astype(jnp.bfloat16)

    def d_copy(i, c):
        return pltpu.make_async_remote_copy(
            src_ref=d_out.at[i, c], dst_ref=d_in.at[i, c],
            send_sem=d_send.at[i, c], recv_sem=d_recv.at[i, c],
            device_id=partner, device_id_type=MESH,
        )

    def b_copy(i, c):
        return pltpu.make_async_remote_copy(
            src_ref=b_out.at[i, c], dst_ref=b_in.at[i, c],
            send_sem=b_send.at[i, c], recv_sem=b_recv.at[i, c],
            device_id={"tensor": (x + i) % X}, device_id_type=MESH,
        )

    def c_copy(d, c):
        return pltpu.make_async_remote_copy(
            src_ref=c_out.at[(e + d) % E, c], dst_ref=c_in.at[d, c],
            send_sem=c_send.at[d, c], recv_sem=c_recv.at[d, c],
            device_id={"expert": (e + d) % E}, device_id_type=MESH,
        )

    def down(i, c):
        w_copies[i, c].wait()
        piece = jnp.dot(hidden, wd[i, c], preferred_element_type=jnp.float32)
        d_out[i, c] = piece[half:].astype(jnp.bfloat16)
        copy = d_copy(i, c)
        copy.start()
        sent.append(copy)
        keep[i, c] = piece[:half]

    def over_tensor(i, c):
        d_copy(i, c).wait_recv()
        both = keep[i, c] + d_in[i, c].astype(jnp.float32)
        if i:
            b_out[i, c] = both.astype(jnp.bfloat16)
            copy = b_copy(i, c)
            copy.start()
            sent.append(copy)
        else:
            for d in range(1, X):
                b_copy(d, c).wait_recv()
                both = both + b_in[d, c].astype(jnp.float32)
            both = both.astype(jnp.bfloat16)
            for j in range(E):
                c_out[j, c] = both[j * T:(j + 1) * T]
            for d in range(1, E):
                copy = c_copy(d, c)
                copy.start()
                sent.append(copy)

    for i, c in order:
        down(i, c)
    for i, c in order:
        over_tensor(i, c)

    ids_copy.wait()
    codes_copy.wait()
    weight = codes_v[...].astype(jnp.float32) / 64.0
    diagonal = lax.broadcasted_iota(jnp.int32, (T, T), 0) == lax.broadcasted_iota(jnp.int32, (T, T), 1)
    shares = []
    for d in range(E):
        expert = ((e + E - d) % E) // 2
        share = jnp.sum(jnp.where(ids_v[...] == expert, weight, 0.0), axis=0, keepdims=True)
        shares.append(jnp.sum(jnp.where(diagonal, share, 0.0), axis=1, keepdims=True))
    for c in range(C):
        total = shares[0] * c_out[e, c].astype(jnp.float32)
        for d in range(1, E):
            c_copy(d, c).wait_recv()
            total = total + shares[d] * c_in[d, c].astype(jnp.float32)
        out_ref[:, pl.ds(c * cw, cw)] = total.astype(jnp.bfloat16)
    for copy in sent:
        copy.wait_send()


def shards(tokens, expert_ids, gate_codes, w_gate, w_up, w_down):
    T, D = tokens.shape
    E = lax.axis_size("expert")
    X = lax.axis_size("tensor")
    F = w_gate.shape[1]
    K = split_count(D, 4)
    block = D // X
    C = split_count(block, 4)
    kw, cw = D // K, block // C
    half = E * T
    bf16, f32 = jnp.bfloat16, jnp.float32
    dma = pltpu.SemaphoreType.DMA
    hbm = pl.BlockSpec(memory_space=pltpu.HBM)
    return pl.pallas_call(
        functools.partial(layer, E, X, K, C),
        out_shape=jax.ShapeDtypeStruct((T, block), bf16),
        in_specs=[hbm] * 6,
        out_specs=pl.BlockSpec(memory_space=pltpu.VMEM),
        scratch_shapes=[
            pltpu.VMEM((2, E, T, D), bf16),
            pltpu.VMEM((2 * half, D), bf16),
            pltpu.VMEM(expert_ids.shape[::-1], jnp.int32),
            pltpu.VMEM(gate_codes.shape[::-1], jnp.int32),
            pltpu.VMEM((K, F, kw), bf16),
            pltpu.VMEM((K, F, kw), bf16),
            pltpu.VMEM((X, C, F, cw), bf16),
            pltpu.VMEM((X, C, half, cw), f32),
            pltpu.VMEM((X, C, half, cw), bf16),
            pltpu.VMEM((X, C, half, cw), bf16),
            pltpu.VMEM((X, C, half, cw), bf16),
            pltpu.VMEM((X, C, half, cw), bf16),
            pltpu.VMEM((E, C, T, cw), bf16),
            pltpu.VMEM((E, C, T, cw), bf16),
            dma((3,)), dma((K,)), dma((K,)), dma((X, C)),
            dma((E, K)), dma((E, K)), dma((E, K)), dma((E, K)),
            dma((X, C)), dma((X, C)), dma((X, C)), dma((X, C)),
            dma((E, C)), dma((E, C)),
        ],
        compiler_params=pltpu.CompilerParams(
            collective_id=0, has_side_effects=True, vmem_limit_bytes=67043328 - 44 * 1024
        ),
    )(tokens, expert_ids.T, gate_codes.T, w_gate, w_up, w_down)


def solution(mesh):
    return jax.shard_map(
        shards,
        mesh=mesh,
        in_specs=(
            P(("group", "expert", "sub"), None),
            P(("group", "expert", "sub"), None),
            P(("group", "expert", "sub"), None),
            P("expert", ("tensor", "sub"), None),
            P("expert", ("tensor", "sub"), None),
            P("expert", ("tensor", "sub"), None),
        ),
        out_specs=P(("group", "expert", "sub"), "tensor"),
        check_vma=False,
    )
```

```python
import functools

import jax
import jax.numpy as jnp
from jax import lax
from jax.experimental import pallas as pl
from jax.experimental.pallas import tpu as pltpu
from jax.sharding import PartitionSpec as P

MESH = pl.DeviceIdType.MESH


def split_count(width, most):
    parts = most
    while width % (parts * 128):
        parts -= 1
    return parts


def layer(
    E, X, K, C,
    tok_hbm, ids_hbm, codes_hbm, wg_hbm, wu_hbm, wd_hbm,
    out_ref,
    gat, xs, ids_v, codes_v, wg, wu, wd,
    keep, d_out, d_in, b_out, b_in, c_out, c_in,
    small_sem, wg_sem, wu_sem, wd_sem,
    z_send, z_recv, f_send, f_recv, d_send, d_recv, b_send, b_recv, c_send, c_recv,
):
    T, D = tok_hbm.shape
    half = E * T
    kw = D // K
    block = D // X
    cw = block // C
    e = lax.axis_index("expert")
    x = lax.axis_index("tensor")
    s = lax.axis_index("sub")
    partner = {"sub": 1 - s}

    barrier = pltpu.get_barrier_semaphore()
    for d in range(1, E):
        pl.semaphore_signal(barrier, inc=1, device_id={"expert": (e + d) % E}, device_id_type=MESH)
    for d in range(1, X):
        pl.semaphore_signal(barrier, inc=1, device_id={"tensor": (x + d) % X}, device_id_type=MESH)
    pl.semaphore_signal(barrier, inc=1, device_id=partner, device_id_type=MESH)

    tok_copy = pltpu.make_async_copy(tok_hbm, gat.at[0, e], small_sem.at[0])
    tok_copy.start()
    ids_copy = pltpu.make_async_copy(ids_hbm, ids_v, small_sem.at[1])
    codes_copy = pltpu.make_async_copy(codes_hbm, codes_v, small_sem.at[2])
    ids_copy.start()
    codes_copy.start()

    g_copies, u_copies, w_copies = [], [], {}
    for k in range(K):
        cols = pl.ds(k * kw, kw)
        g_copies.append(pltpu.make_async_copy(wg_hbm.at[0, :, cols], wg.at[k], wg_sem.at[k]))
        u_copies.append(pltpu.make_async_copy(wu_hbm.at[0, :, cols], wu.at[k], wu_sem.at[k]))
        g_copies[k].start()
        u_copies[k].start()
    order = [(i, c) for i in list(range(1, X)) + [0] for c in range(C)]
    for i, c in order:
        first = pl.multiple_of(((x + i) % X) * block + c * cw, 128)
        w_copies[i, c] = pltpu.make_async_copy(
            wd_hbm.at[0, :, pl.ds(first, cw)], wd.at[i, c], wd_sem.at[i, c]
        )
        w_copies[i, c].start()

    tok_copy.wait()
    pl.semaphore_wait(barrier, E - 1 + X - 1 + 1)

    def z_copy(d, k, slot):
        piece = gat.at[0, slot, :, pl.ds(k * kw, kw)]
        return pltpu.make_async_remote_copy(
            src_ref=piece, dst_ref=piece, send_sem=z_send.at[d, k], recv_sem=z_recv.at[d, k],
            device_id={"expert": (e + d) % E}, device_id_type=MESH,
        )

    def f_copy(d, k):
        slot = (e + E - d) % E
        cols = pl.ds(k * kw, kw)
        return pltpu.make_async_remote_copy(
            src_ref=gat.at[0, slot, :, cols], dst_ref=gat.at[1, slot, :, cols],
            send_sem=f_send.at[d, k], recv_sem=f_recv.at[d, k],
            device_id=partner, device_id_type=MESH,
        )

    sent = []
    for k in range(K):
        for d in range(1, E):
            copy = z_copy(d, k, e)
            copy.start()
            sent.append(copy)
        copy = f_copy(0, k)
        copy.start()
        sent.append(copy)

    def forward(k):
        for d in range(1, E):
            z_copy(d, k, (e + E - d) % E).wait_recv()
            copy = f_copy(d, k)
            copy.start()
            sent.append(copy)

    contract = (((1,), (1,)), ((), ()))
    gate_act = up_act = None
    forward(0)
    for k in range(K):
        if k + 1 < K:
            forward(k + 1)
        for d in range(E):
            f_copy(d, k).wait_recv()
        for r in range(2):
            for j in range(E):
                xs[pl.ds((r * E + j) * T, T), pl.ds(k * kw, kw)] = gat[r, j, :, pl.ds(k * kw, kw)]
        rows = xs[:, pl.ds(k * kw, kw)]
        g_copies[k].wait()
        gate_part = lax.dot_general(rows, wg[k], contract, preferred_element_type=jnp.float32)
        u_copies[k].wait()
        up_part = lax.dot_general(rows, wu[k], contract, preferred_element_type=jnp.float32)
        gate_act = gate_part if k == 0 else gate_act + gate_part
        up_act = up_part if k == 0 else up_act + up_part
    hidden = (gate_act / (1.0 + jnp.exp(-gate_act)) * up_act).astype(jnp.bfloat16)

    def d_copy(i, c):
        return pltpu.make_async_remote_copy(
            src_ref=d_out.at[i, c], dst_ref=d_in.at[i, c],
            send_sem=d_send.at[i, c], recv_sem=d_recv.at[i, c],
            device_id=partner, device_id_type=MESH,
        )

    def b_copy(i, c):
        return pltpu.make_async_remote_copy(
            src_ref=b_out.at[i, c], dst_ref=b_in.at[i, c],
            send_sem=b_send.at[i, c], recv_sem=b_recv.at[i, c],
            device_id={"tensor": (x + i) % X}, device_id_type=MESH,
        )

    def c_copy(d, c):
        return pltpu.make_async_remote_copy(
            src_ref=c_out.at[(e + d) % E, c], dst_ref=c_in.at[d, c],
            send_sem=c_send.at[d, c], recv_sem=c_recv.at[d, c],
            device_id={"expert": (e + d) % E}, device_id_type=MESH,
        )

    def down(i, c):
        w_copies[i, c].wait()
        piece = jnp.dot(hidden, wd[i, c], preferred_element_type=jnp.float32)
        d_out[i, c] = piece[half:].astype(jnp.bfloat16)
        copy = d_copy(i, c)
        copy.start()
        sent.append(copy)
        keep[i, c] = piece[:half]

    def over_tensor(i, c):
        d_copy(i, c).wait_recv()
        both = keep[i, c] + d_in[i, c].astype(jnp.float32)
        if i:
            b_out[i, c] = both.astype(jnp.bfloat16)
            copy = b_copy(i, c)
            copy.start()
            sent.append(copy)
        else:
            for d in range(1, X):
                b_copy(d, c).wait_recv()
                both = both + b_in[d, c].astype(jnp.float32)
            both = both.astype(jnp.bfloat16)
            for j in range(E):
                c_out[j, c] = both[j * T:(j + 1) * T]
            for d in range(1, E):
                copy = c_copy(d, c)
                copy.start()
                sent.append(copy)

    for i, c in order:
        down(i, c)
    for i, c in order:
        over_tensor(i, c)

    ids_copy.wait()
    codes_copy.wait()
    weight = codes_v[...].astype(jnp.float32) / 64.0
    diagonal = lax.broadcasted_iota(jnp.int32, (T, T), 0) == lax.broadcasted_iota(jnp.int32, (T, T), 1)
    shares = []
    for d in range(E):
        expert = ((e + E - d) % E) // 2
        share = jnp.sum(jnp.where(ids_v[...] == expert, weight, 0.0), axis=0, keepdims=True)
        shares.append(jnp.sum(jnp.where(diagonal, share, 0.0), axis=1, keepdims=True))
    for c in range(C):
        total = shares[0] * c_out[e, c].astype(jnp.float32)
        for d in range(1, E):
            c_copy(d, c).wait_recv()
            total = total + shares[d] * c_in[d, c].astype(jnp.float32)
        out_ref[:, pl.ds(c * cw, cw)] = total.astype(jnp.bfloat16)
    for copy in sent:
        copy.wait_send()


def shards(tokens, expert_ids, gate_codes, w_gate, w_up, w_down):
    T, D = tokens.shape
    E = lax.axis_size("expert")
    X = lax.axis_size("tensor")
    F = w_gate.shape[1]
    K = split_count(D, 4)
    block = D // X
    C = split_count(block, 2)
    kw, cw = D // K, block // C
    half = E * T
    bf16, f32 = jnp.bfloat16, jnp.float32
    dma = pltpu.SemaphoreType.DMA
    hbm = pl.BlockSpec(memory_space=pltpu.HBM)
    return pl.pallas_call(
        functools.partial(layer, E, X, K, C),
        out_shape=jax.ShapeDtypeStruct((T, block), bf16),
        in_specs=[hbm] * 6,
        out_specs=pl.BlockSpec(memory_space=pltpu.VMEM),
        scratch_shapes=[
            pltpu.VMEM((2, E, T, D), bf16),
            pltpu.VMEM((2 * half, D), bf16),
            pltpu.VMEM(expert_ids.shape[::-1], jnp.int32),
            pltpu.VMEM(gate_codes.shape[::-1], jnp.int32),
            pltpu.VMEM((K, F, kw), bf16),
            pltpu.VMEM((K, F, kw), bf16),
            pltpu.VMEM((X, C, F, cw), bf16),
            pltpu.VMEM((X, C, half, cw), f32),
            pltpu.VMEM((X, C, half, cw), bf16),
            pltpu.VMEM((X, C, half, cw), bf16),
            pltpu.VMEM((X, C, half, cw), bf16),
            pltpu.VMEM((X, C, half, cw), bf16),
            pltpu.VMEM((E, C, T, cw), bf16),
            pltpu.VMEM((E, C, T, cw), bf16),
            dma((3,)), dma((K,)), dma((K,)), dma((X, C)),
            dma((E, K)), dma((E, K)), dma((E, K)), dma((E, K)),
            dma((X, C)), dma((X, C)), dma((X, C)), dma((X, C)),
            dma((E, C)), dma((E, C)),
        ],
        compiler_params=pltpu.CompilerParams(
            collective_id=0, has_side_effects=True, vmem_limit_bytes=67043328 - 44 * 1024
        ),
    )(tokens, expert_ids.T, gate_codes.T, w_gate, w_up, w_down)


def solution(mesh):
    return jax.shard_map(
        shards,
        mesh=mesh,
        in_specs=(
            P(("group", "expert", "sub"), None),
            P(("group", "expert", "sub"), None),
            P(("group", "expert", "sub"), None),
            P("expert", ("tensor", "sub"), None),
            P("expert", ("tensor", "sub"), None),
            P("expert", ("tensor", "sub"), None),
        ),
        out_specs=P(("group", "expert", "sub"), "tensor"),
        check_vma=False,
    )
```
